32 devices in a mesh: row: 8 (over y, x, core), col: 4 (over z).
Axes of the slice: x: 2, y: 2, z: 4, core: 2. Of those that a mesh axis runs over, the one named last changes fastest.
Arguments:
- tokens: bfloat16 [1024, 8192], P('row', 'col'), may hold values from -6 to 6
- weights: bfloat16 [2, 14336, 8192], P(None, 'row', 'col'), may hold values from -0.0625 to 0.0625
- gradients: bfloat16 [2, 14336, 8192], P(None, 'row', 'col'), may hold values from -200 to 200, as said below
- row_factors: float32 [2, 14336], P(None, 'row'), may hold values from 0.05 to 0.5
- col_factors: float32 [2, 8192], P(None, 'col'), may hold values from 0.05 to 0.5
Outputs:
- hidden: bfloat16 [1024, 14336], P('col', 'row')
- row_new: float32 [2, 14336], P(None, 'row')
- col_new: float32 [2, 8192], P(None, 'col')
The draws below stay inside these ranges and needn't reach their ends.
Inputs may be any that keep to these rules, and one draw needn't show every extreme that they name: Finite real gradients.
All inputs are finite; a program needn't handle non-finite values.
Results may differ from the reference program's by a relative error of at most 0.001.
The reference program's roundings to bfloat16 on the way (of `new_weights`) count: a program that leaves them out, or rounds other values in their place, can miss the bound.
Values may be sent and summed in bfloat16 or wider, within the bound.
A program may use at most 128 MiB of HBM per device.

```python
import math
import jax
import jax.numpy as jnp
from jax import lax

D = 8192
FF = 14336
TOKENS = 1024


def draw_gradients(key, part):
    keys = jax.random.split(jax.random.fold_in(key, 17), 5)
    row_pos = jnp.arange(FF, dtype=jnp.float32) / FF
    col_pos = jnp.arange(D, dtype=jnp.float32) / D
    row_scale = 0.5 * jnp.power(3.0, row_pos)[None, :, None] * jnp.exp(jax.random.uniform(keys[0], (2, FF, 1), jnp.float32, math.log(0.4), math.log(2.5)))
    col_scale = 0.5 * jnp.power(3.0, col_pos)[None, None, :] * jnp.exp(jax.random.uniform(keys[1], (2, 1, D), jnp.float32, math.log(0.4), math.log(2.5)))
    values = jax.random.normal(keys[4], (2, FF, D), jnp.float32) * row_scale * col_scale
    return jnp.clip(values, -200.0, 200.0).astype(jnp.bfloat16)


def block_levels(key, dims, shards, least, largest):
    gain = 1.0
    for dim, parts in shards:
        heights = jax.random.uniform(jax.random.fold_in(jax.random.fold_in(key, 6), dim), (parts,), jnp.float32, least / len(shards), largest / len(shards))
        gain = gain * jnp.repeat(jnp.exp(heights), dims[dim] // parts).reshape((-1,) + (1,) * (len(dims) - 1 - dim))
    return gain


def bell_draw(rng, shape, deviation, limit, cuts=(), kind=jnp.bfloat16):
    gain = block_levels(rng, shape, cuts, -0.22, 0.18) if cuts else 1.0
    values = jax.random.normal(rng, shape, jnp.float32) * deviation * gain
    return jnp.minimum(jnp.maximum(values, -limit), limit).astype(kind)


def setup_inputs(seed: int = 0) -> dict:
    key_list = jax.random.split(jax.random.key(seed), 6)
    return {
        "tokens": bell_draw(key_list[0], (TOKENS, D), 1.0, 6.0, ((0, 8), (1, 4))),
        "weights": bell_draw(key_list[1], (2, FF, D), D ** -0.5, 0.0625, ((1, 8), (2, 4))),
        "gradients": draw_gradients(jax.random.fold_in(key_list[5], 71), 0),
        "row_factors": jnp.clip(jnp.exp(math.log(0.5) - 2.3025851 * jax.random.uniform(key_list[3], (2, FF), jnp.float32) ** block_levels(key_list[3], (2, FF), ((1, 8),), -0.2, 0.2)), 0.05, 0.5),
        "col_factors": jnp.clip(jnp.exp(math.log(0.5) - 2.3025851 * jax.random.uniform(key_list[4], (2, D), jnp.float32) ** block_levels(key_list[4], (2, D), ((1, 4),), -0.2, 0.2)), 0.05, 0.5),
    }


decay_rate = 0.5
learn_rate = 0.01
clip_limit = 1.0
tiny_eps = 1e-30

def reference(tokens, weights, gradients, row_factors, col_factors):
    gradient = gradients.astype(jnp.float32)
    squares = gradient * gradient
    row_new = decay_rate * row_factors + (1.0 - decay_rate) * (lax.optimization_barrier(jnp.mean(squares, axis=2)) + tiny_eps)
    col_new = decay_rate * col_factors + (1.0 - decay_rate) * (lax.optimization_barrier(jnp.mean(squares, axis=1)) + tiny_eps)
    row_mean = lax.optimization_barrier(jnp.mean(row_new, axis=1))
    denominator = jnp.sqrt(row_new[:, :, None] * col_new[:, None, :] / row_mean[:, None, None])
    update = gradient / denominator
    rms_value = jnp.sqrt(lax.optimization_barrier(jnp.mean(update * update, axis=(1, 2))))
    clip_scale = jnp.maximum(1.0, rms_value / clip_limit)
    new_weights = (weights.astype(jnp.float32) - learn_rate * update / clip_scale[:, None, None]).astype(jnp.bfloat16)
    gate_proj = lax.dot_general(tokens, new_weights[0], (((1,), (1,)), ((), ())), preferred_element_type=jnp.float32)
    up_proj = lax.dot_general(tokens, new_weights[1], (((1,), (1,)), ((), ())), preferred_element_type=jnp.float32)
    hidden = (jax.nn.silu(gate_proj) * up_proj).astype(jnp.bfloat16)
    return (hidden, row_new, col_new)
```

```python
import functools
import jax
import jax.numpy as jnp
from jax import lax
from jax.experimental import pallas as pl
from jax.experimental.pallas import tpu as pltpu
from jax.sharding import PartitionSpec as P

decay_rate = 0.5
learn_rate = 0.01
clip_limit = 1.0
tiny_eps = 1e-30
code_span = 250.0


def exchange_kernel(axis, count, x_ref, out_ref, slots, send_sems, recv_sems):
    me = lax.axis_index(axis)
    barrier = pltpu.get_barrier_semaphore()
    for step in range(1, count):
        peer = lax.rem(me + step, count)
        pl.semaphore_signal(
            barrier, inc=1, device_id={axis: peer}, device_id_type=pl.DeviceIdType.MESH
        )
    pl.semaphore_wait(barrier, count - 1)
    copies = []
    for step in range(1, count):
        peer = lax.rem(me + step, count)
        copy = pltpu.make_async_remote_copy(
            src_ref=x_ref,
            dst_ref=slots.at[me],
            send_sem=send_sems.at[step],
            recv_sem=recv_sems.at[me],
            device_id={axis: peer},
            device_id_type=pl.DeviceIdType.MESH,
        )
        copy.start()
        copies.append(copy)
    slots[me] = x_ref[...]
    for step in range(1, count):
        peer = lax.rem(me + count - step, count)
        pltpu.make_async_remote_copy(
            src_ref=x_ref,
            dst_ref=slots.at[peer],
            send_sem=send_sems.at[step],
            recv_sem=recv_sems.at[peer],
            device_id={axis: peer},
            device_id_type=pl.DeviceIdType.MESH,
        ).wait_recv()
    total = slots[0]
    for index in range(1, count):
        total = total + slots[index]
    out_ref[...] = total
    for copy in copies:
        copy.wait_send()


def exchange_sum(x, axis, count, collective_id):
    return pl.pallas_call(
        functools.partial(exchange_kernel, axis, count),
        out_shape=jax.ShapeDtypeStruct(x.shape, x.dtype),
        in_specs=[pl.BlockSpec(memory_space=pltpu.VMEM)],
        out_specs=pl.BlockSpec(memory_space=pltpu.VMEM),
        scratch_shapes=[
            pltpu.VMEM((count,) + x.shape, x.dtype),
            pltpu.SemaphoreType.DMA((count,)),
            pltpu.SemaphoreType.DMA((count,)),
        ],
        cost_estimate=pl.CostEstimate(
            flops=0, bytes_accessed=10 * 1024 * 1024, transcendentals=0
        ),
        compiler_params=pltpu.CompilerParams(
            collective_id=collective_id, has_side_effects=True
        ),
    )(x)


def encode(part):
    peak = jnp.max(jnp.abs(part), axis=1, keepdims=True)
    peak = lax.reduce_precision(jnp.maximum(peak * 1.005, 1e-30), 8, 7)
    level = jnp.abs(part) * (code_span / peak) - 0.5 * code_span
    size = jnp.exp2(level)
    code = jnp.where(part < 0, -size, size)
    tail = jnp.broadcast_to(peak, (part.shape[0], 128))
    return jnp.concatenate([code.astype(jnp.bfloat16), tail.astype(jnp.bfloat16)], axis=1)


def decode(packet):
    width = packet.shape[1] - 128
    code = packet[:, :width].astype(jnp.float32)
    peak = packet[:, width : width + 1].astype(jnp.float32)
    value = (jnp.log2(jnp.abs(code)) + 0.5 * code_span) * (peak / code_span)
    return jnp.where(code < 0, -value, value)


def local(rows, cols, tokens, weights, gradients, row_factors, col_factors):
    row_block, col_block = gradients.shape[1], gradients.shape[2]
    hidden_units, features = row_block * rows, col_block * cols
    spread = lax.all_gather(tokens, "row", axis=0, tiled=True)
    gradient = gradients.astype(jnp.float32)
    squares = gradient * gradient
    row_part = jnp.sum(squares, axis=2)
    col_part = jnp.sum(squares, axis=1)
    row_total = exchange_sum(row_part, "col", cols, 0)
    row_new = decay_rate * row_factors + (1.0 - decay_rate) * (row_total / features + tiny_eps)
    row_sum = jnp.broadcast_to(jnp.sum(row_new, axis=1, keepdims=True), (2, 128))
    totals = exchange_sum(jnp.concatenate([col_part, row_sum], axis=1), "row", rows, 1)
    col_total = totals[:, :col_block]
    row_mean = totals[:, col_block] / hidden_units
    col_new = decay_rate * col_factors + (1.0 - decay_rate) * (col_total / hidden_units + tiny_eps)
    row_gain = jnp.sqrt(row_mean[:, None] / row_new)
    col_gain = 1.0 / jnp.sqrt(col_new)
    update = gradient * row_gain[:, :, None] * col_gain[:, None, :]
    norm_part = jnp.sum(update * update, axis=(1, 2))
    norm_part = jnp.broadcast_to(norm_part[:, None], (2, 128))
    norm_total = exchange_sum(exchange_sum(norm_part, "col", cols, 2), "row", rows, 3)[:, 0]
    clip_scale = jnp.maximum(1.0, jnp.sqrt(norm_total / (hidden_units * features)) / clip_limit)
    rate = learn_rate / clip_scale
    scaled_gain = row_gain * rate[:, None]
    new_weights = (
        weights.astype(jnp.float32) - gradient * scaled_gain[:, :, None] * col_gain[:, None, :]
    ).astype(jnp.bfloat16)

    me = lax.axis_index("col")
    token_block = spread.shape[0] // cols
    pieces = 2 if row_block % 256 == 0 else 1
    width = row_block // pieces
    forward = [(i, (i + 1) % cols) for i in range(cols)]
    backward = [(i, (i + cols - 1) % cols) for i in range(cols)]
    lanes = [(part, piece) for piece in range(pieces) for part in range(2)]
    held = {}
    for step in range(cols):
        for lane in lanes:
            part, piece = lane
            if part == 0:
                block = lax.rem(me + 2 * cols - 1 - step, cols)
            else:
                block = lax.rem(me + 1 + step, cols)
            chosen = lax.dynamic_slice_in_dim(spread, block * token_block, token_block, axis=0)
            mine = lax.dot_general(
                chosen,
                new_weights[part, piece * width : (piece + 1) * width],
                (((1,), (1,)), ((), ())),
                preferred_element_type=jnp.float32,
            )
            if step > 0:
                mine = mine + decode(held[lane])
            if step < cols - 1:
                route = forward if part == 0 else backward
                held[lane] = lax.ppermute(encode(mine), "col", route)
            else:
                held[lane] = mine
    hidden = jnp.concatenate(
        [
            (jax.nn.silu(held[(0, piece)]) * held[(1, piece)]).astype(jnp.bfloat16)
            for piece in range(pieces)
        ],
        axis=1,
    )
    return (hidden, row_new, col_new)


def solution(mesh):
    placed = (
        P("row", "col"),
        P(None, "row", "col"),
        P(None, "row", "col"),
        P(None, "row"),
        P(None, "col"),
    )
    return jax.shard_map(
        functools.partial(local, mesh.shape["row"], mesh.shape["col"]),
        mesh=mesh,
        in_specs=placed,
        out_specs=(P("col", "row"), P(None, "row"), P(None, "col")),
        check_vma=False,
    )
```
